32 devices in a mesh: row: 8 (over z, core), col: 4 (over y, x).
Axes of the slice: x: 2, y: 2, z: 4, core: 2. Of those that a mesh axis runs over, the one named last changes fastest.
Arguments:
- df_blocks: bfloat16 [576, 576, 1024], P('row', 'col'), may hold values from -1 to 1
- amplitudes: bfloat16 [48, 576, 576], P(None, 'col'), may hold values from -0.009765625 to 0.009765625
Outputs:
- ladder_ab: float32 [576, 4, 48], P('row')
- ladder_ba: float32 [576, 4, 48], P('row')
The draws below stay inside these ranges and needn't reach their ends.
All inputs are finite; a program needn't handle non-finite values.
Results may differ from the reference program's by a relative error of at most 0.0029.
Values may be sent and summed in bfloat16 or wider, within the bound.
A program may use at most 192 MiB of HBM per device.

```python
import jax
import jax.numpy as jnp
from jax import lax

NV = 576
NAUX = 1024
WIN = 4
PAIRS = 48
N_ROW = 8


def block_scale(own_key, dims, split, smallest, largest):
    def one(position, parts):
        steps = jax.random.uniform(jax.random.fold_in(jax.random.fold_in(own_key, 6), position), (parts,), jnp.float32, smallest / len(split), largest / len(split))
        return jnp.repeat(jnp.exp(steps), dims[position] // parts).reshape((-1,) + (1,) * (len(dims) - position - 1))

    loudness = one(*split[0])
    for cut in split[1:]:
        loudness = loudness * one(*cut)
    return loudness


def noise(key, extent, width, reach, cuts=(), held_as=jnp.bfloat16):
    drawn = jax.random.normal(key, extent, jnp.float32) * width
    if len(cuts) > 0:
        drawn = block_scale(key, extent, cuts, -0.22, 0.18) * drawn
    return jnp.clip(drawn, min=-reach, max=reach).astype(held_as)


def setup_inputs(seed: int = 0) -> dict:
    seeds = jax.random.split(jax.random.key(seed), 3)
    return {
        "df_blocks": noise(seeds[0], (NV, NV, NAUX), 32 ** -0.5, 1.0, ((0, 8), (1, 4))),
        "amplitudes": noise(seeds[1], (PAIRS, NV, NV), (NV * NV) ** -0.5, 0.009765625, ((1, 4),)),
    }


def reference(df_blocks, amplitudes):
    own_rows = NV // N_ROW
    blocks = df_blocks.reshape(N_ROW, own_rows, NV, NAUX)
    partner = jnp.roll(blocks[:, :WIN], -1, axis=0)
    amps_wide = amplitudes.astype(jnp.float32)

    def ladder_block(block_pair):
        resident, window_rows = block_pair
        v_tile = jnp.einsum("acq,jdq->ajcd", resident.astype(jnp.float32), window_rows.astype(jnp.float32), precision=lax.Precision.HIGHEST)
        v_tile = lax.optimization_barrier(v_tile.astype(jnp.bfloat16)).astype(jnp.float32)
        forward = jnp.einsum("ajcd,pcd->ajp", v_tile, amps_wide, precision=lax.Precision.HIGHEST)
        backward = jnp.einsum("ajcd,pdc->ajp", v_tile, amps_wide, precision=lax.Precision.HIGHEST)
        return forward, backward

    forward, backward = lax.map(ladder_block, (blocks, partner))
    return forward.reshape(NV, WIN, PAIRS), backward.reshape(NV, WIN, PAIRS)
```

```python
import functools

import jax
import jax.numpy as jnp
from jax import lax
from jax.experimental import pallas as pl
from jax.experimental.pallas import tpu as pltpu
from jax.sharding import PartitionSpec as P

WIN = 4
LANES = 128
NT = (((1,), (1,)), ((), ()))


def shifted_2(value, axis, steps):
    count = lax.axis_size(axis)
    pairs = [(source, (source + steps) % count) for source in range(count)]
    return lax.ppermute(value, axis, pairs)


def ladder_kernel(rows, whole, rest, rows_ref, window_ref, amps_ref, out_ref, tile):
    group = amps_ref.shape[0]

    @pl.when(pl.program_id(0) == 0)
    def _():
        out_ref[...] = jnp.zeros_like(out_ref)

    resident = rows_ref[...]

    def one(j, carry):
        at = pl.multiple_of(j * whole, LANES)
        tile[:, pl.ds(at, whole)] = lax.dot_general(
            resident, window_ref[pl.ds(at, whole), :], NT, preferred_element_type=jnp.float32
        )
        return carry

    lax.fori_loop(0, WIN, one, 0)
    if rest:
        tile[:, WIN * whole:] = lax.dot_general(
            resident, window_ref[WIN * whole:, :], NT, preferred_element_type=jnp.float32
        )
        owner = lax.broadcasted_iota(jnp.int32, (rows, WIN * rest), 1) // rest
    total = out_ref[...]
    for c in range(group):
        at = slice(c * rows, (c + 1) * rows)
        parts = []
        for j in range(WIN):
            part = tile[at, j * whole:(j + 1) * whole]
            if rest:
                tail = jnp.where(owner == j, tile[at, WIN * whole:], 0.0)
                part = jnp.concatenate([part, tail], axis=1)
            parts.append(part)
        stacked = jnp.concatenate(parts, axis=0).astype(jnp.bfloat16)
        total += lax.dot_general(stacked, amps_ref[c], NT, preferred_element_type=jnp.float32)
    out_ref[...] = total


def ladder(by_c, window, amps, group):
    columns, rows, depth = by_c.shape
    pairs2, width = amps.shape[1:]
    extent = window.shape[0] // WIN
    whole = extent // LANES * LANES
    rest = extent - whole
    flat = by_c.reshape(columns * rows, depth)
    return pl.pallas_call(
        functools.partial(ladder_kernel, rows, whole, rest),
        grid=(columns // group,),
        out_shape=jax.ShapeDtypeStruct((WIN * rows, pairs2), jnp.float32),
        in_specs=[
            pl.BlockSpec((group * rows, depth), lambda i: (i, 0)),
            pl.BlockSpec((WIN * extent, depth), lambda i: (0, 0)),
            pl.BlockSpec((group, pairs2, width), lambda i: (i, 0, 0)),
        ],
        out_specs=pl.BlockSpec((WIN * rows, pairs2), lambda i: (0, 0)),
        scratch_shapes=[pltpu.VMEM((group * rows, WIN * extent), jnp.float32)],
        compiler_params=pltpu.CompilerParams(
            dimension_semantics=("arbitrary",), vmem_limit_bytes=60 * 1024 * 1024
        ),
        cost_estimate=pl.CostEstimate(
            flops=2 * columns * rows * WIN * extent * (depth + pairs2),
            bytes_accessed=2 * (flat.size + window.size + amps.size),
            transcendentals=0,
        ),
    )(flat, window, amps)


NN = pl.DeviceIdType.MESH
GROUP = 16
SHARES = 4


def matmul_nt(lhs, rhs):
    return lax.dot_general(lhs, rhs, NT, preferred_element_type=jnp.float32)


def fused_kernel(
    row_count, col_count, df_ref, amps_ref, flip_ref, flip_tail_ref, out_ref,
    slabs, window, tiled, direct, direct_tail, flipped, flipped_tail, stage_b, stage_t, parts,
    own_s, own_r, near_s, near_r, far_s, far_r, share_s, share_r, relay_s, relay_r, pair_s, pair_r,
    tail_s, tail_r, sum_s, sum_r, local, stage_b_sem, stage_t_sem,
):
    rows, columns, depth = df_ref.shape
    pairs = amps_ref.shape[0]
    extra = columns - LANES
    chunks = columns // GROUP
    span = GROUP * rows
    share = columns // SHARES
    octets = flip_tail_ref.shape[0] // col_count
    r, q = lax.axis_index("row"), lax.axis_index("col")
    below, above = lax.rem(r + row_count - 1, row_count), lax.rem(r + 1, row_count)
    slot_r = lax.rem(r, SHARES)
    odd = lax.rem(r, 2)
    mate = r + 1 - 2 * odd
    upper = lax.rem(r // 2, 2)
    twin = r + 2 - 4 * upper
    qx, qy = lax.rem(q, 2), q // 2
    x_q = qy * 2 + (1 - qx)
    y_q = (1 - qy) * 2 + qx
    d_q = (1 - qy) * 2 + (1 - qx)
    peers = (q, x_q, y_q, d_q)

    def remote(src, dst, send, recv, dr, dq):
        return pltpu.make_async_remote_copy(
            src_ref=src, dst_ref=dst, send_sem=send, recv_sem=recv, device_id=(dr, dq), device_id_type=NN
        )

    def own(j):
        return remote(df_ref.at[j], window.at[0, j], own_s.at[j], own_r.at[j], below, q)

    def near(k, j):
        return remote(window.at[0, j], window.at[k, j], near_s.at[k - 1, j], near_r.at[k - 1, j], r, peers[k])

    def far(j):
        k = 1 if j < 2 else 2
        return remote(window.at[k, j], window.at[3, j], far_s.at[j], far_r.at[j], r, peers[3 - k])

    def share_at(s):
        return pl.ds(s * share, share)

    def shared(k):
        src = flip_ref.at[pl.ds(peers[k] * columns + slot_r * share, share)]
        return remote(src, flipped.at[k, share_at(slot_r)], share_s.at[k - 1], share_r.at[k - 1], r, peers[k])

    def relay(k):
        ref = flipped.at[k, share_at(slot_r)]
        return remote(ref, ref, relay_s.at[k - 1], relay_r.at[k - 1], twin, q)

    def pair(k, h):
        s = slot_r if h == 0 else lax.rem(twin, SHARES)
        ref = flipped.at[k, share_at(s)]
        return remote(ref, ref, pair_s.at[k - 1, h], pair_r.at[k - 1, h], mate, q)

    def tails(k):
        src = flip_tail_ref.at[pl.ds(peers[k] * octets, octets)]
        return remote(src, flipped_tail.at[k], tail_s.at[k - 1], tail_r.at[k - 1], r, peers[k])

    def sums(k):
        return remote(out_ref, parts.at[k - 1], sum_s.at[k - 1], sum_r.at[k - 1], r, peers[k])

    def fetch_b(i, slot):
        at = pl.multiple_of(i * GROUP, GROUP)
        return pltpu.make_async_copy(df_ref.at[:, pl.ds(at, GROUP), :], stage_b.at[slot], stage_b_sem.at[slot])

    def fetch_t(i, slot):
        at = pl.multiple_of(i * GROUP, GROUP)
        return pltpu.make_async_copy(amps_ref.at[:, pl.ds(at, GROUP), :], stage_t.at[slot], stage_t_sem.at[slot])

    fetch_t(0, 0).start()
    fetch_b(0, 0).start()
    own_flip = pltpu.make_async_copy(flip_ref.at[pl.ds(q * columns, columns)], flipped.at[0], local.at[0])
    own_tail = pltpu.make_async_copy(flip_tail_ref.at[pl.ds(q * octets, octets)], flipped_tail.at[0], local.at[1])
    own_flip.start()
    own_tail.start()

    barrier = pltpu.get_barrier_semaphore()
    for dr, dq in ((below, q), (above, q), (twin, q), (r, x_q), (r, y_q), (r, d_q)):
        pl.semaphore_signal(barrier, inc=1, device_id=(dr, dq), device_id_type=NN)
    pl.semaphore_wait(barrier, 6)

    for j in range(WIN):
        own(j).start()
    shared(1).start()
    shared(2).start()

    def prepare_t(i, carry):
        slot = lax.rem(i, 2)
        fetch_t(i, slot).wait()

        @pl.when(i + 1 < chunks)
        def _():
            fetch_t(i + 1, 1 - slot).start()

        by_c = jnp.swapaxes(stage_t[slot], 0, 1)
        at = pl.multiple_of(i * GROUP, GROUP)
        for o in range(col_count):
            direct[o, pl.ds(at, GROUP)] = by_c[:, :, o * columns:o * columns + LANES]
        for t in range(GROUP // 4):
            direct_tail[i * (GROUP // 4) + t] = jnp.concatenate(
                [
                    by_c[4 * t + c, :, o * columns + LANES:(o + 1) * columns]
                    for c in range(4) for o in range(col_count)
                ],
                axis=1,
            )
        return carry

    lax.fori_loop(0, chunks, prepare_t, 0)

    for j in range(WIN):
        own(j).wait_recv()
        near(1, j).start()
        near(2, j).start()
    shared(3).start()
    own_flip.wait()
    own_tail.wait()

    def prepare_b(i, carry):
        slot = lax.rem(i, 2)
        fetch_b(i, slot).wait()

        @pl.when(i + 1 < chunks)
        def _():
            fetch_b(i + 1, 1 - slot).start()

        by_c = jnp.swapaxes(stage_b[slot].astype(jnp.float32), 0, 1).reshape(span, depth)
        slabs[pl.ds(pl.multiple_of(i * span, LANES), span), :] = by_c.astype(jnp.bfloat16)
        return carry

    lax.fori_loop(0, chunks, prepare_b, 0)
    out_ref[...] = jnp.zeros_like(out_ref)

    def piece(k, carry):
        @pl.when(k == 1)
        def _():
            for j in range(WIN):
                near(1, j).wait_recv()
                near(2, j).wait_recv()
            for j in range(WIN):
                far(j).start()
            for p in range(1, 4):
                tails(p).start()
            for p in range(1, 4):
                relay(p).wait_recv()
                pair(p, 0).start()
                pair(p, 1).start()
            for h in range(2):
                pair(1, h).wait_recv()

        @pl.when(k == 2)
        def _():
            for h in range(2):
                pair(2, h).wait_recv()

        @pl.when(k == 3)
        def _():
            for j in range(WIN):
                far(j).wait_recv()
            for h in range(2):
                pair(3, h).wait_recv()

        kx, ky = lax.rem(k, 2), k // 2
        origin = (qy + ky - 2 * qy * ky) * 2 + (qx + kx - 2 * qx * kx)

        def chunk(i, inner):
            @pl.when((k == 0) & (i == chunks // 2))
            def _():
                for p in range(1, 4):
                    shared(p).wait_recv()
                    relay(p).start()

            lhs = slabs[pl.ds(pl.multiple_of(i * span, LANES), span), :]
            rhs = jnp.concatenate([window[k, j, :LANES, :] for j in range(WIN)], axis=0)
            tiled[...] = matmul_nt(lhs, rhs)
            total = out_ref[...]
            for c in range(0, GROUP, 2):
                at = i * GROUP + c
                stacked = jnp.concatenate(
                    [
                        jnp.concatenate(
                            [
                                tiled[(c + h) * rows:(c + h + 1) * rows, j * LANES:(j + 1) * LANES]
                                for h in range(2)
                            ],
                            axis=1,
                        )
                        for j in range(WIN)
                    ],
                    axis=0,
                ).astype(jnp.bfloat16)
                both = jnp.concatenate(
                    [
                        jnp.concatenate([direct[origin, at], direct[origin, at + 1]], axis=1),
                        jnp.concatenate([flipped[k, at], flipped[k, at + 1]], axis=1),
                    ],
                    axis=0,
                )
                total += matmul_nt(stacked, both)
            out_ref[...] = total
            return inner

        lax.fori_loop(0, chunks, chunk, 0)
        return carry

    lax.fori_loop(0, col_count, piece, 0)

    for k in range(1, 4):
        tails(k).wait_recv()
    step = WIN * extra

    def place(o):
        kx, ky = o % 2, o // 2
        return (qy + ky - 2 * qy * ky) * 2 + (qx + kx - 2 * qx * kx)

    def tail_chunk(i, carry):
        lhs = slabs[pl.ds(pl.multiple_of(i * span, LANES), span), :]
        rhs = jnp.concatenate(
            [window[place(o), j, LANES:, :] for j in range(WIN) for o in range(col_count)], axis=0
        )
        tiled[:, :WIN * step] = matmul_nt(lhs, rhs)
        total = out_ref[...]
        for t in range(GROUP // 4):
            stacked = jnp.concatenate(
                [
                    jnp.concatenate(
                        [
                            tiled[(4 * t + c) * rows:(4 * t + c + 1) * rows, j * step:(j + 1) * step]
                            for c in range(4)
                        ],
                        axis=1,
                    )
                    for j in range(WIN)
                ],
                axis=0,
            ).astype(jnp.bfloat16)
            first = 4 * (t % 2)
            back = jnp.concatenate(
                [
                    flipped_tail[place(o), i * (GROUP // 8) + t // 2, :, (first + c) * extra:(first + c + 1) * extra]
                    for c in range(4) for o in range(col_count)
                ],
                axis=1,
            )
            both = jnp.concatenate([direct_tail[i * (GROUP // 4) + t], back], axis=0)
            total += matmul_nt(stacked, both)
        out_ref[...] = total
        return carry

    lax.fori_loop(0, chunks, tail_chunk, 0)

    for k in range(1, 4):
        sums(k).start()
    for j in range(WIN):
        own(j).wait_send()
        near(1, j).wait_send()
        near(2, j).wait_send()
        far(j).wait_send()
    for k in range(1, 4):
        shared(k).wait_send()
        relay(k).wait_send()
        pair(k, 0).wait_send()
        pair(k, 1).wait_send()
        tails(k).wait_send()
    for k in range(1, 4):
        sums(k).wait()
    out_ref[...] = (out_ref[...] + parts[0]) + (parts[1] + parts[2])


def fused(df_blocks, amplitudes):
    rows, columns, depth = df_blocks.shape
    pairs, _, extent = amplitudes.shape
    row_count, col_count = lax.axis_size("row"), lax.axis_size("col")
    extra = columns - LANES
    flip = amplitudes[:, :LANES, :].transpose(2, 0, 1)
    flip_tail = amplitudes[:, LANES:, :].reshape(pairs, extra, extent // 8, 8)
    flip_tail = flip_tail.transpose(2, 0, 3, 1).reshape(extent // 8, pairs, 8 * extra)
    dma = pltpu.SemaphoreType.DMA
    bf16 = jnp.bfloat16
    total = pl.pallas_call(
        functools.partial(fused_kernel, row_count, col_count),
        out_shape=jax.ShapeDtypeStruct((WIN * rows, 2 * pairs), jnp.float32),
        in_specs=[pl.BlockSpec(memory_space=pltpu.HBM)] * 4,
        out_specs=pl.BlockSpec(memory_space=pltpu.VMEM),
        scratch_shapes=[
            pltpu.VMEM((columns * rows, depth), bf16),
            pltpu.VMEM((col_count, WIN, columns, depth), bf16),
            pltpu.VMEM((GROUP * rows, WIN * LANES), jnp.float32),
            pltpu.VMEM((col_count, columns, pairs, LANES), bf16),
            pltpu.VMEM((columns // 4, pairs, 4 * col_count * extra), bf16),
            pltpu.VMEM((col_count, columns, pairs, LANES), bf16),
            pltpu.VMEM((col_count, columns // 8, pairs, LANES), bf16),
            pltpu.VMEM((2, rows, GROUP, depth), bf16),
            pltpu.VMEM((2, pairs, GROUP, extent), bf16),
            pltpu.VMEM((3, WIN * rows, 2 * pairs), jnp.float32),
            dma((4,)), dma((4,)), dma((2, 4)), dma((2, 4)), dma((4,)), dma((4,)),
            dma((3,)), dma((3,)), dma((3,)), dma((3,)), dma((3, 2)), dma((3, 2)),
            dma((3,)), dma((3,)), dma((3,)), dma((3,)), dma((2,)), dma((2,)), dma((2,)),
        ],
        compiler_params=pltpu.CompilerParams(
            collective_id=0, has_side_effects=True, vmem_limit_bytes=67043328
        ),
    )(df_blocks, amplitudes, flip, flip_tail)
    total = total.reshape(WIN, rows, 2 * pairs).transpose(1, 0, 2)
    return (total[:, :, :pairs], total[:, :, pairs:])


def fits_fused(df_blocks, amplitudes):
    rows, columns, depth = df_blocks.shape
    pairs, _, extent = amplitudes.shape
    row_count, col_count = lax.axis_size("row"), lax.axis_size("col")
    extra = columns - LANES
    return (
        col_count == 4 and row_count % SHARES == 0 and row_count >= 4 and rows % 8 == 0 and rows >= WIN
        and columns % GROUP == 0 and columns % SHARES == 0 and extra == 16 and WIN == 4
        and pairs % 16 == 0 and depth % LANES == 0 and GROUP * rows % LANES == 0
    )


def shards(df_blocks, amplitudes):
    if fits_fused(df_blocks, amplitudes):
        return fused(df_blocks, amplitudes)
    rows, columns, depth = df_blocks.shape
    pairs, _, extent = amplitudes.shape
    row_count = lax.axis_size("row")
    shifted = shifted_2(df_blocks[:WIN], "row", -1)
    window = lax.all_gather(shifted, "col", axis=1, tiled=True)
    if pairs % row_count == 0:
        share = pairs // row_count
        own = lax.dynamic_slice_in_dim(amplitudes, lax.axis_index("row") * share, share, 0)
        own = lax.all_to_all(own, "col", split_axis=2, concat_axis=1, tiled=True)
        own = own.transpose(0, 2, 1)
        flipped = lax.all_gather(own, "row", axis=0, tiled=True).transpose(1, 0, 2)
    else:
        flipped = lax.all_to_all(amplitudes, "col", split_axis=2, concat_axis=1, tiled=True)
        flipped = flipped.transpose(2, 0, 1)
    amps = jnp.concatenate([amplitudes.transpose(1, 0, 2), flipped], axis=1)
    whole = extent // LANES * LANES
    if extent > whole:
        amps = jnp.concatenate([amps[:, :, :whole]] + [amps[:, :, whole:]] * WIN, axis=2)
        window = jnp.concatenate(
            [window[:, :whole].reshape(-1, depth), window[:, whole:].reshape(-1, depth)], axis=0
        )
    else:
        window = window.reshape(-1, depth)
    by_c = df_blocks.transpose(1, 0, 2)
    group = next(g for g in (8, 6, 4, 2, 1) if columns % g == 0 and (g * rows % 16 == 0 or g == 1))
    total = ladder(by_c, window, amps, group)
    total = lax.psum(total, "col").reshape(WIN, rows, 2 * pairs).transpose(1, 0, 2)
    return (total[:, :, :pairs], total[:, :, pairs:])


def solution(mesh):
    in_specs = (P("row", "col", None), P(None, "col", None))
    out_specs = (P("row", None, None), P("row", None, None))
    return jax.shard_map(shards, mesh=mesh, in_specs=in_specs, out_specs=out_specs, check_vma=False)
```

```python
import functools

import jax
import jax.numpy as jnp
from jax import lax
from jax.experimental import pallas as pl
from jax.experimental.pallas import tpu as pltpu
from jax.sharding import PartitionSpec as P

WIN = 4
LANES = 128
NT = (((1,), (1,)), ((), ()))


def shifted_2(value, axis, steps):
    count = lax.axis_size(axis)
    pairs = [(source, (source + steps) % count) for source in range(count)]
    return lax.ppermute(value, axis, pairs)


def ladder_kernel(rows, whole, rest, rows_ref, window_ref, amps_ref, out_ref, tile):
    group = amps_ref.shape[0]

    @pl.when(pl.program_id(0) == 0)
    def _():
        out_ref[...] = jnp.zeros_like(out_ref)

    resident = rows_ref[...]

    def one(j, carry):
        at = pl.multiple_of(j * whole, LANES)
        tile[:, pl.ds(at, whole)] = lax.dot_general(
            resident, window_ref[pl.ds(at, whole), :], NT, preferred_element_type=jnp.float32
        )
        return carry

    lax.fori_loop(0, WIN, one, 0)
    if rest:
        tile[:, WIN * whole:] = lax.dot_general(
            resident, window_ref[WIN * whole:, :], NT, preferred_element_type=jnp.float32
        )
        owner = lax.broadcasted_iota(jnp.int32, (rows, WIN * rest), 1) // rest
    total = out_ref[...]
    for c in range(group):
        at = slice(c * rows, (c + 1) * rows)
        parts = []
        for j in range(WIN):
            part = tile[at, j * whole:(j + 1) * whole]
            if rest:
                tail = jnp.where(owner == j, tile[at, WIN * whole:], 0.0)
                part = jnp.concatenate([part, tail], axis=1)
            parts.append(part)
        stacked = jnp.concatenate(parts, axis=0).astype(jnp.bfloat16)
        total += lax.dot_general(stacked, amps_ref[c], NT, preferred_element_type=jnp.float32)
    out_ref[...] = total


def ladder(by_c, window, amps, group):
    columns, rows, depth = by_c.shape
    pairs2, width = amps.shape[1:]
    extent = window.shape[0] // WIN
    whole = extent // LANES * LANES
    rest = extent - whole
    flat = by_c.reshape(columns * rows, depth)
    return pl.pallas_call(
        functools.partial(ladder_kernel, rows, whole, rest),
        grid=(columns // group,),
        out_shape=jax.ShapeDtypeStruct((WIN * rows, pairs2), jnp.float32),
        in_specs=[
            pl.BlockSpec((group * rows, depth), lambda i: (i, 0)),
            pl.BlockSpec((WIN * extent, depth), lambda i: (0, 0)),
            pl.BlockSpec((group, pairs2, width), lambda i: (i, 0, 0)),
        ],
        out_specs=pl.BlockSpec((WIN * rows, pairs2), lambda i: (0, 0)),
        scratch_shapes=[pltpu.VMEM((group * rows, WIN * extent), jnp.float32)],
        compiler_params=pltpu.CompilerParams(
            dimension_semantics=("arbitrary",), vmem_limit_bytes=60 * 1024 * 1024
        ),
        cost_estimate=pl.CostEstimate(
            flops=2 * columns * rows * WIN * extent * (depth + pairs2),
            bytes_accessed=2 * (flat.size + window.size + amps.size),
            transcendentals=0,
        ),
    )(flat, window, amps)


NN = pl.DeviceIdType.MESH
GROUP = 16
SHARES = 4


def matmul_nt(lhs, rhs):
    return lax.dot_general(lhs, rhs, NT, preferred_element_type=jnp.float32)


def fused_kernel(
    row_count, col_count, df_ref, amps_ref, out_ref,
    slabs, window, tiled, direct, direct_tail, flipped, flipped_tail, flip_out, tail_out, stage_b, stage_t, stage_f, parts,
    own_s, own_r, near_s, near_r, far_s, far_r, share_s, share_r, relay_s, relay_r, pair_s, pair_r,
    sum_s, sum_r, stage_b_sem, stage_t_sem, stage_f_sem,
):
    rows, columns, depth = df_ref.shape
    pairs = amps_ref.shape[0]
    extra = columns - LANES
    chunks = columns // GROUP
    span = GROUP * rows
    extent = amps_ref.shape[2]
    octets = columns // 8
    share = pairs // SHARES
    padded = flip_out.shape[1]
    r, q = lax.axis_index("row"), lax.axis_index("col")
    below, above = lax.rem(r + row_count - 1, row_count), lax.rem(r + 1, row_count)
    slot_r = lax.rem(r, SHARES)
    odd = lax.rem(r, 2)
    mate = r + 1 - 2 * odd
    upper = lax.rem(r // 2, 2)
    twin = r + 2 - 4 * upper
    qx, qy = lax.rem(q, 2), q // 2
    x_q = qy * 2 + (1 - qx)
    y_q = (1 - qy) * 2 + qx
    d_q = (1 - qy) * 2 + (1 - qx)
    peers = (q, x_q, y_q, d_q)

    def remote(src, dst, send, recv, dr, dq):
        return pltpu.make_async_remote_copy(
            src_ref=src, dst_ref=dst, send_sem=send, recv_sem=recv, device_id=(dr, dq), device_id_type=NN
        )

    def own(j):
        return remote(df_ref.at[j], window.at[0, j], own_s.at[j], own_r.at[j], below, q)

    def near(k, j):
        return remote(window.at[0, j], window.at[k, j], near_s.at[k - 1, j], near_r.at[k - 1, j], r, peers[k])

    def far(j):
        k = 1 if j < 2 else 2
        return remote(window.at[k, j], window.at[3, j], far_s.at[j], far_r.at[j], r, peers[3 - k])

    def at_share(s):
        return pl.ds(pl.multiple_of(s * padded, padded), padded)

    def both_parts(k, make):
        return (make(flipped.at[k], 0), make(flipped_tail.at[k], 1))

    def shared(k):
        def make(ref, t):
            size = octets if t else columns
            src = (tail_out if t else flip_out).at[pl.ds(peers[k] * size, size)]
            dst = ref.at[:, at_share(slot_r), :]
            return remote(src, dst, share_s.at[k - 1, t], share_r.at[k - 1, t], r, peers[k])
        return both_parts(k, make)

    def relay(k):
        def make(ref, t):
            ref = ref.at[:, at_share(slot_r), :]
            return remote(ref, ref, relay_s.at[k, t], relay_r.at[k, t], twin, q)
        return both_parts(k, make)

    def pair(k, h):
        s = slot_r if h == 0 else lax.rem(twin, SHARES)

        def make(ref, t):
            ref = ref.at[:, at_share(s), :]
            return remote(ref, ref, pair_s.at[k, h, t], pair_r.at[k, h, t], mate, q)
        return both_parts(k, make)

    def start(copies):
        for copy in copies:
            copy.start()

    def wait_recv(copies):
        for copy in copies:
            copy.wait_recv()

    def wait_send(copies):
        for copy in copies:
            copy.wait_send()

    def sums(k):
        return remote(out_ref, parts.at[k - 1], sum_s.at[k - 1], sum_r.at[k - 1], r, peers[k])

    def fetch_b(i, slot):
        at = pl.multiple_of(i * GROUP, GROUP)
        return pltpu.make_async_copy(df_ref.at[:, pl.ds(at, GROUP), :], stage_b.at[slot], stage_b_sem.at[slot])

    def fetch_t(i, slot):
        at = pl.multiple_of(i * GROUP, GROUP)
        return pltpu.make_async_copy(amps_ref.at[:, pl.ds(at, GROUP), :], stage_t.at[slot], stage_t_sem.at[slot])

    fetch_t(0, 0).start()
    fetch_b(0, 0).start()
    fetch_f = pltpu.make_async_copy(amps_ref.at[pl.ds(slot_r * share, share)], stage_f, stage_f_sem.at[0])
    fetch_f.start()

    barrier = pltpu.get_barrier_semaphore()
    for dr, dq in ((below, q), (above, q), (twin, q), (r, x_q), (r, y_q), (r, d_q)):
        pl.semaphore_signal(barrier, inc=1, device_id=(dr, dq), device_id_type=NN)
    pl.semaphore_wait(barrier, 6)

    for j in range(WIN):
        own(j).start()
    fetch_f.wait()
    blank = jnp.zeros((extent, columns), jnp.bfloat16)
    for at in range(0, extent, LANES):
        size = min(LANES, extent - at)
        turned = jnp.stack(
            [stage_f[p, :, at:at + size].T for p in range(share)] + [blank[:size]] * (padded - share), axis=0
        )
        by_d = jnp.swapaxes(turned, 0, 1)
        flip_out[at:at + size] = by_d[:, :, :LANES]
        for o in range(size // 8):
            tail_out[at // 8 + o] = jnp.concatenate([by_d[8 * o + c, :, LANES:] for c in range(8)], axis=1)
    flipped[0, :, at_share(slot_r), :] = flip_out[pl.ds(q * columns, columns)]
    flipped_tail[0, :, at_share(slot_r), :] = tail_out[pl.ds(q * octets, octets)]

    def forward_window():
        for j in range(WIN):
            own(j).wait_recv()
            near(1, j).start()
            near(2, j).start()

    start(relay(0))
    start(shared(1))
    start(shared(2))

    @pl.when(odd == 0)
    def _():
        forward_window()

    def prepare_t(i, carry):
        slot = lax.rem(i, 2)
        fetch_t(i, slot).wait()

        @pl.when(i + 1 < chunks)
        def _():
            fetch_t(i + 1, 1 - slot).start()

        by_c = jnp.swapaxes(stage_t[slot], 0, 1)
        at = pl.multiple_of(i * GROUP, GROUP)
        for o in range(col_count):
            direct[o, pl.ds(at, GROUP)] = by_c[:, :, o * columns:o * columns + LANES]
        for t in range(GROUP // 4):
            direct_tail[i * (GROUP // 4) + t] = jnp.concatenate(
                [
                    by_c[4 * t + c, :, o * columns + LANES:(o + 1) * columns]
                    for c in range(4) for o in range(col_count)
                ],
                axis=1,
            )
        return carry

    lax.fori_loop(0, chunks, prepare_t, 0)

    @pl.when(odd == 1)
    def _():
        forward_window()

    start(shared(3))

    def prepare_b(i, carry):
        slot = lax.rem(i, 2)
        fetch_b(i, slot).wait()

        @pl.when(i + 1 < chunks)
        def _():
            fetch_b(i + 1, 1 - slot).start()

        by_c = jnp.swapaxes(stage_b[slot].astype(jnp.float32), 0, 1).reshape(span, depth)
        slabs[pl.ds(pl.multiple_of(i * span, LANES), span), :] = by_c.astype(jnp.bfloat16)
        return carry

    lax.fori_loop(0, chunks, prepare_b, 0)
    wait_recv(relay(0))
    for h in range(2):
        start(pair(0, h))
    for p in (1, 2):
        wait_recv(shared(p))
        start(relay(p))
    for h in range(2):
        wait_recv(pair(0, h))
    out_ref[...] = jnp.zeros_like(out_ref)

    def piece(k, carry):
        @pl.when(k == 1)
        def _():
            for j in range(WIN):
                near(1, j).wait_recv()
                near(2, j).wait_recv()
            for j in range(WIN):
                far(j).start()
            for h in range(2):
                wait_recv(pair(1, h))

        @pl.when(k == 2)
        def _():
            for h in range(2):
                wait_recv(pair(2, h))

        @pl.when(k == 3)
        def _():
            for j in range(WIN):
                far(j).wait_recv()
            for h in range(2):
                wait_recv(pair(3, h))

        kx, ky = lax.rem(k, 2), k // 2
        origin = (qy + ky - 2 * qy * ky) * 2 + (qx + kx - 2 * qx * kx)

        def chunk(i, inner):
            @pl.when((k == 0) & (i == chunks - 2))
            def _():
                for p in (1, 2):
                    wait_recv(relay(p))
                    for h in range(2):
                        start(pair(p, h))

            @pl.when((k == 1) & (i == chunks - 3))
            def _():
                wait_recv(shared(3))
                start(relay(3))

            @pl.when((k == 2) & (i == chunks - 2))
            def _():
                wait_recv(relay(3))
                for h in range(2):
                    start(pair(3, h))

            lhs = slabs[pl.ds(pl.multiple_of(i * span, LANES), span), :]
            rhs = jnp.concatenate([window[k, j, :LANES, :] for j in range(WIN)], axis=0)
            tiled[...] = matmul_nt(lhs, rhs)
            total = None
            for c in range(0, GROUP, 2):
                at = i * GROUP + c
                stacked = jnp.concatenate(
                    [
                        jnp.concatenate(
                            [
                                tiled[(c + h) * rows:(c + h + 1) * rows, j * LANES:(j + 1) * LANES]
                                for h in range(2)
                            ],
                            axis=1,
                        )
                        for j in range(WIN)
                    ],
                    axis=0,
                ).astype(jnp.bfloat16)
                both = jnp.concatenate(
                    [
                        jnp.concatenate([direct[origin, at], direct[origin, at + 1]], axis=1),
                        jnp.concatenate([flipped[k, at], flipped[k, at + 1]], axis=1),
                    ],
                    axis=0,
                )
                term = matmul_nt(stacked, both)
                total = term if total is None else total + term
            out_ref[...] += total
            return inner

        lax.fori_loop(0, chunks, chunk, 0)
        return carry

    lax.fori_loop(0, col_count, piece, 0)

    step = WIN * extra

    def place(o):
        kx, ky = o % 2, o // 2
        return (qy + ky - 2 * qy * ky) * 2 + (qx + kx - 2 * qx * kx)

    def tail_chunk(i, carry):
        lhs = slabs[pl.ds(pl.multiple_of(i * span, LANES), span), :]
        rhs = jnp.concatenate(
            [window[place(o), j, LANES:, :] for j in range(WIN) for o in range(col_count)], axis=0
        )
        tiled[:, :WIN * step] = matmul_nt(lhs, rhs)
        total = None
        for t in range(GROUP // 4):
            stacked = jnp.concatenate(
                [
                    jnp.concatenate(
                        [
                            tiled[(4 * t + c) * rows:(4 * t + c + 1) * rows, j * step:(j + 1) * step]
                            for c in range(4)
                        ],
                        axis=1,
                    )
                    for j in range(WIN)
                ],
                axis=0,
            ).astype(jnp.bfloat16)
            first = 4 * (t % 2)
            back = jnp.concatenate(
                [
                    flipped_tail[place(o), i * (GROUP // 8) + t // 2, :, (first + c) * extra:(first + c + 1) * extra]
                    for c in range(4) for o in range(col_count)
                ],
                axis=1,
            )
            both = jnp.concatenate([direct_tail[i * (GROUP // 4) + t], back], axis=0)
            term = matmul_nt(stacked, both)
            total = term if total is None else total + term
        out_ref[...] += total
        return carry

    lax.fori_loop(0, chunks, tail_chunk, 0)

    for k in range(1, 4):
        sums(k).start()
    for j in range(WIN):
        own(j).wait_send()
        near(1, j).wait_send()
        near(2, j).wait_send()
        far(j).wait_send()
    for k in range(4):
        wait_send(relay(k))
        wait_send(pair(k, 0))
        wait_send(pair(k, 1))
        if k:
            wait_send(shared(k))
    for k in range(1, 4):
        sums(k).wait()
    out_ref[...] = (out_ref[...] + parts[0]) + (parts[1] + parts[2])


def fused(df_blocks, amplitudes):
    rows, columns, depth = df_blocks.shape
    pairs, _, extent = amplitudes.shape
    row_count, col_count = lax.axis_size("row"), lax.axis_size("col")
    extra = columns - LANES
    padded = -(-(pairs // SHARES) // 16) * 16
    width = pairs + SHARES * padded
    dma = pltpu.SemaphoreType.DMA
    bf16 = jnp.bfloat16
    total = pl.pallas_call(
        functools.partial(fused_kernel, row_count, col_count),
        out_shape=jax.ShapeDtypeStruct((WIN * rows, width), jnp.float32),
        in_specs=[pl.BlockSpec(memory_space=pltpu.HBM)] * 2,
        out_specs=pl.BlockSpec(memory_space=pltpu.VMEM),
        scratch_shapes=[
            pltpu.VMEM((columns * rows, depth), bf16),
            pltpu.VMEM((col_count, WIN, columns, depth), bf16),
            pltpu.VMEM((GROUP * rows, WIN * LANES), jnp.float32),
            pltpu.VMEM((col_count, columns, pairs, LANES), bf16),
            pltpu.VMEM((columns // 4, pairs, 4 * col_count * extra), bf16),
            pltpu.VMEM((col_count, columns, SHARES * padded, LANES), bf16),
            pltpu.VMEM((col_count, columns // 8, SHARES * padded, LANES), bf16),
            pltpu.VMEM((extent, padded, LANES), bf16),
            pltpu.VMEM((extent // 8, padded, LANES), bf16),
            pltpu.VMEM((2, rows, GROUP, depth), bf16),
            pltpu.VMEM((2, pairs, GROUP, extent), bf16),
            pltpu.VMEM((pairs // SHARES, columns, extent), bf16),
            pltpu.VMEM((3, WIN * rows, width), jnp.float32),
            dma((4,)), dma((4,)), dma((2, 4)), dma((2, 4)), dma((4,)), dma((4,)),
            dma((3, 2)), dma((3, 2)), dma((4, 2)), dma((4, 2)), dma((4, 2, 2)), dma((4, 2, 2)),
            dma((3,)), dma((3,)), dma((2,)), dma((2,)), dma((1,)),
        ],
        compiler_params=pltpu.CompilerParams(
            collective_id=0, has_side_effects=True, vmem_limit_bytes=67043328
        ),
    )(df_blocks, amplitudes)
    total = total.reshape(WIN, rows, width).transpose(1, 0, 2)
    back = total[:, :, pairs:].reshape(rows, WIN, SHARES, padded)[..., :pairs // SHARES]
    return (total[:, :, :pairs], back.reshape(rows, WIN, pairs))


def fits_fused(df_blocks, amplitudes):
    rows, columns, depth = df_blocks.shape
    pairs, _, extent = amplitudes.shape
    row_count, col_count = lax.axis_size("row"), lax.axis_size("col")
    extra = columns - LANES
    return (
        col_count == 4 and row_count % SHARES == 0 and row_count >= 4 and rows % 8 == 0 and rows >= WIN
        and columns % GROUP == 0 and pairs % SHARES == 0 and extent % 64 == 0 and extra == 16 and WIN == 4
        and pairs % 16 == 0 and depth % LANES == 0 and GROUP * rows % LANES == 0
    )


def shards(df_blocks, amplitudes):
    if fits_fused(df_blocks, amplitudes):
        return fused(df_blocks, amplitudes)
    rows, columns, depth = df_blocks.shape
    pairs, _, extent = amplitudes.shape
    row_count = lax.axis_size("row")
    shifted = shifted_2(df_blocks[:WIN], "row", -1)
    window = lax.all_gather(shifted, "col", axis=1, tiled=True)
    if pairs % row_count == 0:
        share = pairs // row_count
        own = lax.dynamic_slice_in_dim(amplitudes, lax.axis_index("row") * share, share, 0)
        own = lax.all_to_all(own, "col", split_axis=2, concat_axis=1, tiled=True)
        own = own.transpose(0, 2, 1)
        flipped = lax.all_gather(own, "row", axis=0, tiled=True).transpose(1, 0, 2)
    else:
        flipped = lax.all_to_all(amplitudes, "col", split_axis=2, concat_axis=1, tiled=True)
        flipped = flipped.transpose(2, 0, 1)
    amps = jnp.concatenate([amplitudes.transpose(1, 0, 2), flipped], axis=1)
    whole = extent // LANES * LANES
    if extent > whole:
        amps = jnp.concatenate([amps[:, :, :whole]] + [amps[:, :, whole:]] * WIN, axis=2)
        window = jnp.concatenate(
            [window[:, :whole].reshape(-1, depth), window[:, whole:].reshape(-1, depth)], axis=0
        )
    else:
        window = window.reshape(-1, depth)
    by_c = df_blocks.transpose(1, 0, 2)
    group = next(g for g in (8, 6, 4, 2, 1) if columns % g == 0 and (g * rows % 16 == 0 or g == 1))
    total = ladder(by_c, window, amps, group)
    total = lax.psum(total, "col").reshape(WIN, rows, 2 * pairs).transpose(1, 0, 2)
    return (total[:, :, :pairs], total[:, :, pairs:])


def solution(mesh):
    in_specs = (P("row", "col", None), P(None, "col", None))
    out_specs = (P("row", None, None), P("row", None, None))
    return jax.shard_map(shards, mesh=mesh, in_specs=in_specs, out_specs=out_specs, check_vma=False)
```
